512 devices in a mesh: rep: 32 (over x, y), shard: 16 (over z, core).
Axes of the slice: x: 4, y: 8, z: 8, core: 2. Of those that a mesh axis runs over, the one named last changes fastest.
Arguments:
- deltas: bfloat16 [32, 2048, 4096], P('rep', 'shard'), may hold values from -6 to 6
- presence: int32 [32], replicated, may hold values from 0 to 1, as said below
- owner_of: int32 [32], replicated, may hold values from 0 to 31, each once
- outer_params: float32 [2048, 4096], P('shard', 'rep'), may hold values from -6 to 6
- momentum: float32 [2048, 4096], P('shard', 'rep'), may hold values from -4 to 4
Outputs:
- new_weights: bfloat16 [2048, 4096], P('shard')
- new_outer: float32 [2048, 4096], P('shard', 'rep')
- new_momentum: float32 [2048, 4096], P('shard', 'rep')
The draws below stay inside these ranges and needn't reach their ends.
Inputs may be any that keep to these rules, and one draw needn't show every extreme that they name: `presence`: at least one replica group is present.
All inputs are finite; a program needn't handle non-finite values.
Results may differ from the reference program's by a relative error of at most 0.0075.
Values may be sent and summed in bfloat16 or wider, within the bound.
A program may use at most 64 MiB of HBM per device.

```python
import jax
import jax.numpy as jnp
from jax import lax

D = 4096
ROWS = 2048
REPS = 32
BLOCK = 128


def draw_presence(key, part):
    first = jax.random.fold_in(key, 11)
    second = jax.random.fold_in(key, 12)
    flags = jax.random.randint(first, (REPS,), 0, 2).astype(jnp.int32)
    chosen = jax.random.randint(second, (), 0, REPS)
    return flags.at[chosen].set(1).astype(jnp.int32)


def raised(drawn, own_key, source, target, shards_of, factor):
    owner, partner = [(jnp.arange(drawn.shape[dim]) // (drawn.shape[dim] // shards_of)).reshape([-1 if axis == dim else 1 for axis in range(drawn.ndim)]) for dim in (source, target)]
    chosen = jax.random.permutation(own_key, shards_of)[partner]
    strong = (owner == chosen) | (owner == (partner + shards_of // 2) % shards_of)
    return jnp.where(strong, factor * drawn, drawn)


def shard_levels(rng, shape, split, smallest, top_value):
    def one(axis_at, parts):
        draws = jax.random.uniform(jax.random.fold_in(jax.random.fold_in(rng, 6), axis_at), (parts,), jnp.float32, smallest / len(split), top_value / len(split))
        return jnp.repeat(jnp.exp(draws), shape[axis_at] // parts).reshape((-1,) + (1,) * (len(shape) - axis_at - 1))

    factor_of = one(*split[0])
    for cut in split[1:]:
        factor_of = factor_of * one(*cut)
    return factor_of


def gaussian(rng, extent, scale, bound, cuts=(), held_as=jnp.bfloat16):
    drawn = jax.random.normal(rng, extent, jnp.float32) * scale
    if len(cuts) > 0:
        drawn = shard_levels(rng, extent, cuts, -0.22, 0.18) * drawn
    return jnp.clip(drawn, min=-bound, max=bound).astype(held_as)


def bell_draw_with(own_key, extent, spread, bound, pieces, heavy, dtype=jnp.bfloat16):
    values = spread * jax.random.normal(own_key, extent, jnp.float32)
    if pieces:
        values = values * shard_levels(own_key, extent, pieces, -0.22, 0.18)
    return jnp.clip(raised(values, jax.random.fold_in(own_key, 3), *heavy), -bound, bound).astype(dtype)


def setup_inputs(seed: int = 0) -> dict:
    key_list = jax.random.split(jax.random.key(seed), 6)
    deltas = bell_draw_with(key_list[0], (REPS, ROWS, D), 1.0, 6.0, ((0, 32), (1, 16)), (0, 2, 32, 2.75))
    presence = draw_presence(jax.random.fold_in(key_list[5], 71), 0)
    owner_of = jax.random.permutation(key_list[2], REPS).astype(jnp.int32)
    outer_params = gaussian(key_list[3], (ROWS, D), 1.0, 6.0, ((0, 16), (1, 32)), jnp.float32)
    momentum = gaussian(key_list[4], (ROWS, D), 0.5, 4.0, ((0, 16), (1, 32)), jnp.float32)
    return {"deltas": deltas, "presence": presence, "owner_of": owner_of, "outer_params": outer_params, "momentum": momentum}


def reference(deltas, presence, owner_of, outer_params, momentum):
    present = presence.astype(jnp.float32)
    count = jnp.sum(present)

    def add_group(total, item):
        flag, delta = item
        return total + flag * delta.astype(jnp.float32), None

    start = jnp.zeros((ROWS, D), jnp.float32)
    total, unused = lax.scan(add_group, start, (present, deltas))
    average = total / count
    blocks = average.reshape(ROWS, REPS, BLOCK)
    slotted = jnp.take(blocks, owner_of.astype(jnp.int32), axis=1).reshape(ROWS, D)
    new_momentum = 0.9 * momentum + slotted
    new_outer = outer_params - 0.7 * (slotted + 0.9 * new_momentum)
    inverse = jnp.argsort(owner_of).astype(jnp.int32)
    natural = jnp.take(new_outer.reshape(ROWS, REPS, BLOCK), inverse, axis=1).reshape(ROWS, D)
    new_weights = natural.astype(jnp.bfloat16)
    return (new_weights, new_outer, new_momentum)
```

```python
import functools

import jax
import jax.numpy as jnp
from jax import lax
from jax.experimental import pallas as pl
from jax.experimental.pallas import tpu as pltpu
from jax.sharding import PartitionSpec as P

MESH = pl.DeviceIdType.MESH
NX, NY = 4, 8
BLOCK = 128
UP = (4, 3, 2, 1)
DOWN = (5, 6, 7, 0)


def kernel(
    deltas, presence, owner_of, outer_in, momentum_in,
    gathered, outer_out, momentum_out,
    delta, buf, near_l, near_r, far, mixed, from_y, to_y,
    outer_v, momentum_v,
    load_sem, far_send, far_recv, l_send, l_recv, r_send, r_recv, y_send, y_recv,
    gy_send, gy_recv, gl_send, gl_recv, gr_send, gr_recv, gf_send, gf_recv,
):
    me = lax.axis_index("rep")
    x = me // NY
    y = me % NY

    def place(dx, dy):
        return ((x + dx) % NX) * NY + (y + dy) % NY

    right, left = place(1, 0), place(NX - 1, 0)

    loads = [
        pltpu.make_async_copy(deltas.at[0, :, b * BLOCK : (b + 1) * BLOCK], delta.at[b], load_sem.at[b])
        for b in range(NX * NY)
    ]
    for load in loads:
        load.start()
    load_outer = pltpu.make_async_copy(outer_in, outer_v, load_sem.at[NX * NY])
    load_momentum = pltpu.make_async_copy(momentum_in, momentum_v, load_sem.at[NX * NY + 1])
    load_outer.start()
    load_momentum.start()

    barrier = pltpu.get_barrier_semaphore()
    partners = [right, left] + [place(0, dy) for dy in range(1, NY)]
    for partner in partners:
        pl.semaphore_signal(barrier, inc=1, device_id={"rep": partner}, device_id_type=MESH)

    present = presence[me].astype(jnp.float32)
    for load in loads:
        load.wait()
    for dx in (2, 1, 3, 0):
        for dy in range(NY):
            block = delta[owner_of[place(dx, dy)]]
            buf[dx, dy] = (block.astype(jnp.float32) * present).astype(jnp.bfloat16)
    pl.semaphore_wait(barrier, len(partners))

    started = []

    def send(src, dst, send_sem, recv_sem, to):
        copy = pltpu.make_async_remote_copy(
            src_ref=src, dst_ref=dst, send_sem=send_sem, recv_sem=recv_sem,
            device_id={"rep": to}, device_id_type=MESH,
        )
        copy.start()
        started.append(copy)
        return copy

    far_copies = {}
    for up, down in zip(UP, DOWN):
        far_copies[up] = send(buf.at[2, up], far.at[up], far_send.at[up], far_recv.at[up], right)
        far_copies[down] = send(buf.at[2, down], far.at[down], far_send.at[down], far_recv.at[down], left)

    count = presence[0]
    for r in range(1, NX * NY):
        count = count + presence[r]

    l_copies, r_copies = {}, {}
    for up, down in zip(UP, DOWN):
        far_copies[up].wait_recv()
        mixed[up] = (far[up].astype(jnp.float32) + buf[1, up].astype(jnp.float32)).astype(jnp.bfloat16)
        l_copies[up] = send(mixed.at[up], near_l.at[up], l_send.at[up], l_recv.at[up], right)
        l_copies[down] = send(buf.at[1, down], near_l.at[down], l_send.at[down], l_recv.at[down], right)
        far_copies[down].wait_recv()
        mixed[down] = (far[down].astype(jnp.float32) + buf[3, down].astype(jnp.float32)).astype(jnp.bfloat16)
        r_copies[down] = send(mixed.at[down], near_r.at[down], r_send.at[down], r_recv.at[down], left)
        r_copies[up] = send(buf.at[3, up], near_r.at[up], r_send.at[up], r_recv.at[up], left)

    y_copies = {}
    own = None
    for pair in zip(UP, DOWN):
        for dy in pair:
            l_copies[dy].wait_recv()
            r_copies[dy].wait_recv()
            total = buf[0, dy].astype(jnp.float32) + (near_l[dy].astype(jnp.float32) + near_r[dy].astype(jnp.float32))
            if dy == 0:
                own = total
            else:
                to_y[dy] = total.astype(jnp.bfloat16)
                y_copies[dy] = send(to_y.at[dy], from_y.at[dy], y_send.at[dy], y_recv.at[dy], place(0, dy))
    total = own
    for dy in (4, 5, 3, 6, 2, 7, 1):
        y_copies[dy].wait_recv()
        total = total + from_y[dy].astype(jnp.float32)

    average = total / count.astype(jnp.float32)
    load_outer.wait()
    load_momentum.wait()
    new_momentum = 0.9 * momentum_v[...] + average
    new_outer = outer_v[...] - 0.7 * (average + 0.9 * new_momentum)
    gathered[me] = new_outer.astype(jnp.bfloat16)

    def row(dx, dy):
        return gathered.at[place(dx, dy)]

    gy_copies, gl_copies, gr_copies, gf_copies = {}, {}, {}, {}
    order = (1, 7, 2, 6, 3, 5, 4)
    for dy in order:
        gy_copies[dy] = send(row(0, 0), row(0, 0), gy_send.at[dy], gy_recv.at[dy], place(0, dy))

    def spread(dy):
        gl_copies[dy] = send(row(0, dy), row(0, dy), gl_send.at[dy], gl_recv.at[dy], right)
        gr_copies[dy] = send(row(0, dy), row(0, dy), gr_send.at[dy], gr_recv.at[dy], left)

    def relay(dy):
        if dy in UP:
            gl_copies[dy].wait_recv()
            gf_copies[dy] = send(row(3, dy), row(3, dy), gf_send.at[dy], gf_recv.at[dy], right)
        else:
            gr_copies[dy].wait_recv()
            gf_copies[dy] = send(row(1, dy), row(1, dy), gf_send.at[dy], gf_recv.at[dy], left)

    spread(0)
    outer_out[...] = new_outer
    momentum_out[...] = new_momentum
    sources = (0,) + order
    for k, dy in enumerate(order):
        gy_copies[NY - dy].wait_recv()
        spread(dy)
        if k >= 2:
            relay(sources[k - 2])
    for dy in sources[len(order) - 2 :]:
        relay(dy)
    for dy in range(NY):
        (gr_copies if dy in UP else gl_copies)[dy].wait_recv()
        gf_copies[dy].wait_recv()

    for copy in started:
        copy.wait_send()


def place_kernel(owner_of, gathered, outer_v, momentum_v, weights_out, outer_out, momentum_out, sems):
    copies = [
        pltpu.make_async_copy(outer_v, outer_out, sems.at[NX * NY]),
        pltpu.make_async_copy(momentum_v, momentum_out, sems.at[NX * NY + 1]),
    ]
    for j in range(NX * NY):
        columns = pl.ds(pl.multiple_of(owner_of[j] * BLOCK, BLOCK), BLOCK)
        copies.append(pltpu.make_async_copy(gathered.at[j], weights_out.at[:, columns], sems.at[j]))
    for copy in copies:
        copy.start()
    for copy in copies:
        copy.wait()


def shards(deltas, presence, owner_of, outer_params, momentum):
    rows, width = deltas.shape[1], deltas.shape[2]
    wide = functools.partial(pltpu.VMEM, dtype=jnp.bfloat16)
    any_space = pl.BlockSpec(memory_space=pl.ANY)
    scalars = pl.BlockSpec(memory_space=pltpu.SMEM)
    vector = pl.BlockSpec(memory_space=pltpu.VMEM)
    sems = pltpu.SemaphoreType.DMA((NY,))
    gathered, new_outer, new_momentum = pl.pallas_call(
        kernel,
        out_shape=(
            pltpu.VMEM((NX * NY, rows, BLOCK), jnp.bfloat16),
            pltpu.VMEM((rows, BLOCK), jnp.float32),
            pltpu.VMEM((rows, BLOCK), jnp.float32),
        ),
        in_specs=[any_space, scalars, scalars, any_space, any_space],
        out_specs=(vector, vector, vector),
        scratch_shapes=[
            wide((NX * NY, rows, BLOCK)),
            wide((NX, NY, rows, BLOCK)),
            wide((NY, rows, BLOCK)),
            wide((NY, rows, BLOCK)),
            wide((NY, rows, BLOCK)),
            wide((NY, rows, BLOCK)),
            wide((NY, rows, BLOCK)),
            wide((NY, rows, BLOCK)),
            pltpu.VMEM((rows, BLOCK), jnp.float32),
            pltpu.VMEM((rows, BLOCK), jnp.float32),
            pltpu.SemaphoreType.DMA((NX * NY + 2,)),
        ]
        + [sems] * 16,
        compiler_params=pltpu.CompilerParams(collective_id=0, has_side_effects=True),
        name="outer_step",
    )(deltas, presence, owner_of, outer_params, momentum)
    in_vmem = functools.partial(pltpu.with_memory_space_constraint, memory_space=pltpu.VMEM)
    return pl.pallas_call(
        place_kernel,
        out_shape=(
            jax.ShapeDtypeStruct((rows, width), jnp.bfloat16),
            jax.ShapeDtypeStruct((rows, BLOCK), jnp.float32),
            jax.ShapeDtypeStruct((rows, BLOCK), jnp.float32),
        ),
        in_specs=[scalars, vector, vector, vector],
        out_specs=(any_space, any_space, any_space),
        scratch_shapes=[pltpu.SemaphoreType.DMA((NX * NY + 2,))],
        name="place_blocks",
    )(owner_of, in_vmem(gathered), in_vmem(new_outer), in_vmem(new_momentum))


def solution(mesh):
    return jax.shard_map(
        shards,
        mesh=mesh,
        in_specs=(P("rep", "shard", None), P(), P(), P("shard", "rep"), P("shard", "rep")),
        out_specs=(P("shard", None), P("shard", "rep"), P("shard", "rep")),
        check_vma=False,
    )
```

```python
import functools

import jax
import jax.numpy as jnp
from jax import lax
from jax.experimental import pallas as pl
from jax.experimental.pallas import tpu as pltpu
from jax.sharding import PartitionSpec as P

SUM_PLAN = ('B', 'F4', 'F3', 'F5', 'F6', 'F2', 'S', 'N4', 'N5', 'N3', 'N6', 'N2', 'T0', 'T4', 'T3', 'T5', 'T2', 'T6', 'M5', 'M3', 'M6', 'M2', 'O', 'Y4', 'Y3', 'Y5', 'Y6', 'Y2')
SPREAD_PLAN = ('f2', 'f6', 'A0', 'f3', 'f5', 'f4', 'f1', 'f7', 'W', 'A6', 'A2', 'G', 'H', 'A5', 'A3', 'A4')
STRAIGHT = (4,)
DIRECT = (4, 3, 5, 2, 6)
MESH = pl.DeviceIdType.MESH
NX, NY = 4, 8
BLOCK = 128
COPIES = 80
UP = (4, 3, 2)
F32, BF16 = jnp.float32, jnp.bfloat16


def kernel(
    deltas, presence, owner_of, outer_in, momentum_in,
    gathered, outer_out, momentum_out,
    delta, buf, side_up, side_down, near_l, near_r, far, mixed, row_out,
    to_y, from_y, outer_v, momentum_v,
    load_sem, send_sems, recv_sems,
):
    me = lax.axis_index("rep")
    x = me // NY
    y = me % NY

    def place(dx, dy):
        return ((x + dx) % NX) * NY + (y + dy) % NY

    right, left = place(1, 0), place(3, 0)
    across, up, down = place(2, 0), place(0, 1), place(0, 7)

    loads = [
        pltpu.make_async_copy(deltas.at[0, :, b * BLOCK : (b + 1) * BLOCK], delta.at[b], load_sem.at[b])
        for b in range(NX * NY)
    ]
    for load in loads:
        load.start()
    load_outer = pltpu.make_async_copy(outer_in, outer_v, load_sem.at[NX * NY])
    load_momentum = pltpu.make_async_copy(momentum_in, momentum_v, load_sem.at[NX * NY + 1])
    load_outer.start()
    load_momentum.start()

    barrier = pltpu.get_barrier_semaphore()
    partners = [right, left, across] + [place(0, dy) for dy in range(1, NY)]
    for partner in partners:
        pl.semaphore_signal(barrier, inc=1, device_id={"rep": partner}, device_id_type=MESH)

    present = presence[me].astype(F32)
    for load in loads:
        load.wait()

    masked = set()

    def term(dy, dx):
        if (dy, dx) not in masked:
            masked.add((dy, dx))
            block = delta[owner_of[place(dx, dy)]]
            buf[dy, dx] = (block.astype(F32) * present).astype(BF16)
        return buf.at[dy, dx]

    started = []

    def send(src, dst, to):
        k = len(started)
        copy = pltpu.make_async_remote_copy(
            src_ref=src, dst_ref=dst, send_sem=send_sems.at[k], recv_sem=recv_sems.at[k],
            device_id={"rep": to}, device_id_type=MESH,
        )
        copy.start()
        started.append(copy)
        return copy

    def drain():
        for copy in started:
            copy.wait_send()

    far_c, l_c, r_c, side_c, own_c, y_c = {}, {}, {}, {}, {}, {}

    def own_row(dx):
        return term(0, dx)[...].astype(F32) + (side_up[dx].astype(F32) + side_down[dx].astype(F32))

    def sum_step(step, dy):
        if step == "B":
            pl.semaphore_wait(barrier, len(partners))
        elif step == "T":
            for dx in range(NX):
                term(dy, dx)
        elif step == "F":
            to = across if dy in STRAIGHT else right if dy in UP else left
            far_c[dy] = send(term(dy, 2), far.at[dy], to)
        elif step == "N":
            if dy in STRAIGHT or dy not in UP:
                l_c[dy] = send(term(dy, 1), near_l.at[dy], right)
            if dy in STRAIGHT or dy in UP:
                r_c[dy] = send(term(dy, 3), near_r.at[dy], left)
        elif step == "M":
            own_term = term(dy, 1 if dy in UP else 3)[...].astype(F32)
            far_c[dy].wait_recv()
            mixed[dy] = (far[dy].astype(F32) + own_term).astype(BF16)
            if dy in UP:
                l_c[dy] = send(mixed.at[dy], near_l.at[dy], right)
            else:
                r_c[dy] = send(mixed.at[dy], near_r.at[dy], left)
        elif step == "S":
            for side, src, dst, to in ((0, 1, side_up, up), (1, 7, side_down, down)):
                for dx in range(NX):
                    term(src, dx)
                side_c[side] = send(buf.at[src], dst, to)
        elif step == "O":
            side_c[0].wait_recv()
            side_c[1].wait_recv()
            for dx, dst, to in ((2, far.at[0], across), (1, near_l.at[0], right), (3, near_r.at[0], left)):
                row_out[dx] = own_row(dx).astype(BF16)
                own_c[dx] = send(row_out.at[dx], dst, to)
        elif step == "Y":
            own_term = term(dy, 0)[...].astype(F32)
            l_c[dy].wait_recv()
            r_c[dy].wait_recv()
            x_total = own_term + (near_l[dy].astype(F32) + near_r[dy].astype(F32))
            if dy in STRAIGHT:
                far_c[dy].wait_recv()
                x_total = x_total + far[dy].astype(F32)
            to_y[dy] = x_total.astype(BF16)
            y_c[dy] = send(to_y.at[dy], from_y.at[dy], place(0, dy))

    for step in SUM_PLAN:
        sum_step(step[0], int(step[1:] or 0))

    count = presence[0]
    for r in range(1, NX * NY):
        count = count + presence[r]
    total = own_row(0)
    load_outer.wait()
    load_momentum.wait()
    for copy in own_c.values():
        copy.wait_recv()
    total = total + (near_l[0].astype(F32) + near_r[0].astype(F32) + far[0].astype(F32))
    for dy, copy in y_c.items():
        copy.wait_recv()
        total = total + from_y[dy].astype(F32)

    average = total / count.astype(F32)
    new_momentum = 0.9 * momentum_v[...] + average
    new_outer = outer_v[...] - 0.7 * (average + 0.9 * new_momentum)
    gathered[me] = new_outer.astype(BF16)

    def row(dx, dy):
        return gathered.at[place(dx, dy)]

    def forward(dx, dy, to):
        return send(row(dx, dy), row(dx, dy), to)

    from_l, from_r, relay_c, across_c, fan_c, sides = {}, {}, {}, {}, {}, []

    def spread_step(step, dy):
        if step == "f":
            fan_c[dy] = forward(0, 0, place(0, dy))
        elif step == "A":
            if dy:
                fan_c[NY - dy].wait_recv()
            from_l[dy] = forward(0, dy, right)
            from_r[dy] = forward(0, dy, left)
            if dy in DIRECT or dy == 0:
                across_c[dy] = forward(0, dy, across)
        elif step == "G":
            from_l[0].wait_recv()
            sides.extend([forward(3, 0, up), forward(3, 0, down)])
            from_r[0].wait_recv()
            sides.extend([forward(1, 0, up), forward(1, 0, down)])
        elif step == "H":
            across_c[0].wait_recv()
            sides.extend([forward(2, 0, up), forward(2, 0, down)])
        elif step == "R":
            if dy in UP:
                from_l[dy].wait_recv()
                relay_c[dy] = forward(3, dy, right)
            else:
                from_r[dy].wait_recv()
                relay_c[dy] = forward(1, dy, left)
        elif step == "W":
            outer_out[...] = new_outer
            momentum_out[...] = new_momentum

    for step in SPREAD_PLAN:
        spread_step(step[0], int(step[1:] or 0))
    fan_c[1].wait_recv()
    fan_c[7].wait_recv()
    for dy in (6, 2, 5, 3, 4):
        if dy in DIRECT:
            from_l[dy].wait_recv()
            from_r[dy].wait_recv()
            across_c[dy].wait_recv()
        else:
            (from_r if dy in UP else from_l)[dy].wait_recv()
            relay_c[dy].wait_recv()
    for copy in sides:
        copy.wait_recv()
    drain()
    assert len(started) <= COPIES


def place_kernel(owner_of, gathered, outer_v, momentum_v, weights_out, outer_out, momentum_out, sems):
    copies = [
        pltpu.make_async_copy(outer_v, outer_out, sems.at[NX * NY]),
        pltpu.make_async_copy(momentum_v, momentum_out, sems.at[NX * NY + 1]),
    ]
    for j in range(NX * NY):
        columns = pl.ds(pl.multiple_of(owner_of[j] * BLOCK, BLOCK), BLOCK)
        copies.append(pltpu.make_async_copy(gathered.at[j], weights_out.at[:, columns], sems.at[j]))
    for copy in copies:
        copy.start()
    for copy in copies:
        copy.wait()


def shards(deltas, presence, owner_of, outer_params, momentum):
    rows, width = deltas.shape[1], deltas.shape[2]
    any_space = pl.BlockSpec(memory_space=pl.ANY)
    scalars = pl.BlockSpec(memory_space=pltpu.SMEM)
    vector = pl.BlockSpec(memory_space=pltpu.VMEM)

    def blocks(*shape, dtype=BF16):
        return pltpu.VMEM((*shape, rows, BLOCK), dtype)

    gathered, new_outer, new_momentum = pl.pallas_call(
        kernel,
        out_shape=(blocks(NX * NY), blocks(dtype=F32), blocks(dtype=F32)),
        in_specs=[any_space, scalars, scalars, any_space, any_space],
        out_specs=(vector, vector, vector),
        scratch_shapes=[
            blocks(NX * NY),
            blocks(NY, NX),
            blocks(NX),
            blocks(NX),
            blocks(NY),
            blocks(NY),
            blocks(NY),
            blocks(NY),
            blocks(NX),
            blocks(NY),
            blocks(NY),
            blocks(dtype=F32),
            blocks(dtype=F32),
            pltpu.SemaphoreType.DMA((NX * NY + 2,)),
            pltpu.SemaphoreType.DMA((COPIES,)),
            pltpu.SemaphoreType.DMA((COPIES,)),
        ],
        compiler_params=pltpu.CompilerParams(collective_id=0, has_side_effects=True),
        name="outer_step",
    )(deltas, presence, owner_of, outer_params, momentum)
    in_vmem = functools.partial(pltpu.with_memory_space_constraint, memory_space=pltpu.VMEM)
    return pl.pallas_call(
        place_kernel,
        out_shape=(
            jax.ShapeDtypeStruct((rows, width), BF16),
            jax.ShapeDtypeStruct((rows, BLOCK), F32),
            jax.ShapeDtypeStruct((rows, BLOCK), F32),
        ),
        in_specs=[scalars, vector, vector, vector],
        out_specs=(any_space, any_space, any_space),
        scratch_shapes=[pltpu.SemaphoreType.DMA((NX * NY + 2,))],
        name="place_blocks",
    )(owner_of, in_vmem(gathered), in_vmem(new_outer), in_vmem(new_momentum))


def solution(mesh):
    return jax.shard_map(
        shards,
        mesh=mesh,
        in_specs=(P("rep", "shard", None), P(), P(), P("shard", "rep"), P("shard", "rep")),
        out_specs=(P("shard", None), P("shard", "rep"), P("shard", "rep")),
        check_vma=False,
    )
```

```python
import functools

import jax
import jax.numpy as jnp
from jax import lax
from jax.experimental import pallas as pl
from jax.experimental.pallas import tpu as pltpu
from jax.sharding import PartitionSpec as P

PLAN = ('F40', 'F30', 'F50', 'F60', 'F20', 'S00', 'N40', 'N50', 'N30', 'N60', 'N20', 'F41', 'F31', 'F51', 'F61', 'F21', 'S01', 'N41', 'N51', 'N31', 'N61', 'N21', 'T00', 'T40', 'T30', 'T50', 'T20', 'T60', 'T01', 'T41', 'T31', 'T51', 'T21', 'T61', 'M50', 'M30', 'M60', 'M20', 'O00', 'Y40', 'M51', 'M31', 'M61', 'M21', 'Y30', 'Y50', 'Y60', 'Y20', 'O01', 'Y41', 'Y31', 'Y51', 'L00', 'Y61', 'Y21', 'D00', 'D01', 'A60', 'A20', 'G00', 'A50', 'A30', 'A40', 'A61', 'A21', 'G01', 'A51', 'A31', 'A41', 'E00', 'E01')
PARTS = 2
MESH = pl.DeviceIdType.MESH
NX, NY = 4, 8
BLOCK = 128
COPIES = 60 * PARTS
UP = (4, 3, 2)
F32, BF16 = jnp.float32, jnp.bfloat16


def kernel(
    deltas, presence, owner_of, outer_in, momentum_in,
    gathered, outer_out, momentum_out,
    delta, buf, side_up, side_down, near_l, near_r, far, mixed, row_out,
    to_y, from_y, outer_v, momentum_v,
    load_sem, send_sems, recv_sems,
):
    me = lax.axis_index("rep")
    x = me // NY
    y = me % NY

    def place(dx, dy):
        return ((x + dx) % NX) * NY + (y + dy) % NY

    right, left = place(1, 0), place(3, 0)
    across, up, down = place(2, 0), place(0, 1), place(0, 7)

    loads = [
        pltpu.make_async_copy(deltas.at[0, :, b * BLOCK : (b + 1) * BLOCK], delta.at[b], load_sem.at[b])
        for b in range(NX * NY)
    ]
    for load in loads:
        load.start()
    load_outer = pltpu.make_async_copy(outer_in, outer_v, load_sem.at[NX * NY])
    load_momentum = pltpu.make_async_copy(momentum_in, momentum_v, load_sem.at[NX * NY + 1])
    load_outer.start()
    load_momentum.start()

    barrier = pltpu.get_barrier_semaphore()
    partners = [right, left, across] + [place(0, dy) for dy in range(1, NY)]
    for partner in partners:
        pl.semaphore_signal(barrier, inc=1, device_id={"rep": partner}, device_id_type=MESH)

    present = presence[me].astype(F32)
    for load in loads:
        load.wait()

    masked = set()
    height = BLOCK // PARTS

    def rows_of(h):
        return pl.ds(h * height, height)

    def term(dy, dx, h):
        rows = rows_of(h)
        if (dy, dx, h) not in masked:
            masked.add((dy, dx, h))
            block = delta[owner_of[place(dx, dy)]][h * height : (h + 1) * height]
            buf[dy, dx, rows] = (block.astype(F32) * present).astype(BF16)
        return buf.at[dy, dx, rows]

    started = []

    def send(src, dst, to):
        k = len(started)
        copy = pltpu.make_async_remote_copy(
            src_ref=src, dst_ref=dst, send_sem=send_sems.at[k], recv_sem=recv_sems.at[k],
            device_id={"rep": to}, device_id_type=MESH,
        )
        copy.start()
        started.append(copy)
        return copy

    def drain():
        for copy in started:
            copy.wait_send()

    c = {}
    count = presence[0]
    for r in range(1, NX * NY):
        count = count + presence[r]

    def wide(ref):
        return ref[...].astype(F32)

    def own_row(dx, h):
        rows = rows_of(h)
        return wide(term(0, dx, h)) + (wide(side_up.at[dx, rows]) + wide(side_down.at[dx, rows]))

    def block_ref(dx, dy, h):
        return gathered.at[place(dx, dy), rows_of(h)]

    def forward(dx, dy, h, to):
        ref = block_ref(dx, dy, h)
        return send(ref, ref, to)

    def spread(dy, h):
        c["right", dy, h] = forward(0, dy, h, right)
        c["left", dy, h] = forward(0, dy, h, left)
        c["across", dy, h] = forward(0, dy, h, across)

    def finish_sum(h):
        rows = rows_of(h)
        total = own_row(0, h)
        for dx in (1, 2, 3):
            c["own", dx, h].wait_recv()
        total = total + (wide(near_l.at[0, rows]) + wide(near_r.at[0, rows]) + wide(far.at[0, rows]))
        for dy in (4, 3, 5, 6, 2):
            c["y", dy, h].wait_recv()
            total = total + wide(from_y.at[dy, rows])
        average = total / count.astype(F32)
        new_momentum = 0.9 * momentum_v[rows] + average
        new_outer = outer_v[rows] - 0.7 * (average + 0.9 * new_momentum)
        gathered[me, rows] = new_outer.astype(BF16)
        for dy in (2, 6, 0, 3, 5, 4, 1, 7):
            if dy:
                c["fan", dy, h] = forward(0, 0, h, place(0, dy))
            else:
                spread(0, h)
        outer_out[rows] = new_outer
        momentum_out[rows] = new_momentum

    def do_step(step, dy, h):
        rows = rows_of(h)
        if step == "F":
            to = across if dy == 4 else right if dy in UP else left
            c["far", dy, h] = send(term(dy, 2, h), far.at[dy, rows], to)
        elif step == "N":
            if dy == 4 or dy not in UP:
                c["l", dy, h] = send(term(dy, 1, h), near_l.at[dy, rows], right)
            if dy in UP:
                c["r", dy, h] = send(term(dy, 3, h), near_r.at[dy, rows], left)
        elif step == "M":
            own_term = wide(term(dy, 1 if dy in UP else 3, h))
            c["far", dy, h].wait_recv()
            mixed[dy, rows] = (wide(far.at[dy, rows]) + own_term).astype(BF16)
            if dy in UP:
                c["l", dy, h] = send(mixed.at[dy, rows], near_l.at[dy, rows], right)
            else:
                c["r", dy, h] = send(mixed.at[dy, rows], near_r.at[dy, rows], left)
        elif step == "S":
            for src, dst, to in ((1, side_up, up), (7, side_down, down)):
                for dx in range(NX):
                    term(src, dx, h)
                c["side", src, h] = send(buf.at[src, :, rows], dst.at[:, rows], to)
        elif step == "O":
            c["side", 1, h].wait_recv()
            c["side", 7, h].wait_recv()
            for dx, dst, to in ((2, far, across), (1, near_l, right), (3, near_r, left)):
                row_out[dx, rows] = own_row(dx, h).astype(BF16)
                c["own", dx, h] = send(row_out.at[dx, rows], dst.at[0, rows], to)
        elif step == "T":
            term(dy, 0, h)
            if dy == 0:
                for dx in range(NX):
                    term(0, dx, h)
            elif dy != 4:
                term(dy, 1 if dy in UP else 3, h)
        elif step == "Y":
            own_term = wide(term(dy, 0, h))
            c["l", dy, h].wait_recv()
            c["r", dy, h].wait_recv()
            x_total = own_term + (wide(near_l.at[dy, rows]) + wide(near_r.at[dy, rows]))
            if dy == 4:
                c["far", dy, h].wait_recv()
                x_total = x_total + wide(far.at[dy, rows])
            to_y[dy, rows] = x_total.astype(BF16)
            c["y", dy, h] = send(to_y.at[dy, rows], from_y.at[dy, rows], place(0, dy))
        elif step == "L":
            load_outer.wait()
            load_momentum.wait()
        elif step == "D":
            finish_sum(h)
        elif step == "A":
            c["fan", NY - dy, h].wait_recv()
            spread(dy, h)
        elif step == "G":
            for name, dx in (("left", 1), ("right", 3), ("across", 2)):
                c[name, 0, h].wait_recv()
                c["side_up", dx, h] = forward(dx, 0, h, up)
                c["side_down", dx, h] = forward(dx, 0, h, down)
        elif step == "E":
            c["fan", 1, h].wait_recv()
            c["fan", 7, h].wait_recv()
            for dy in (6, 2, 5, 3, 4):
                for name in ("right", "left", "across"):
                    c[name, dy, h].wait_recv()
            for dx in (1, 2, 3):
                c["side_up", dx, h].wait_recv()
                c["side_down", dx, h].wait_recv()

    pl.semaphore_wait(barrier, len(partners))
    for token in PLAN:
        do_step(token[0], int(token[1]), int(token[2]))
    drain()
    assert len(started) <= COPIES


def place_kernel(owner_of, gathered, outer_v, momentum_v, weights_out, outer_out, momentum_out, sems):
    copies = [
        pltpu.make_async_copy(outer_v, outer_out, sems.at[NX * NY]),
        pltpu.make_async_copy(momentum_v, momentum_out, sems.at[NX * NY + 1]),
    ]
    for j in range(NX * NY):
        columns = pl.ds(pl.multiple_of(owner_of[j] * BLOCK, BLOCK), BLOCK)
        copies.append(pltpu.make_async_copy(gathered.at[j], weights_out.at[:, columns], sems.at[j]))
    for copy in copies:
        copy.start()
    for copy in copies:
        copy.wait()


def shards(deltas, presence, owner_of, outer_params, momentum):
    rows, width = deltas.shape[1], deltas.shape[2]
    any_space = pl.BlockSpec(memory_space=pl.ANY)
    scalars = pl.BlockSpec(memory_space=pltpu.SMEM)
    vector = pl.BlockSpec(memory_space=pltpu.VMEM)

    def blocks(*shape, dtype=BF16):
        return pltpu.VMEM((*shape, rows, BLOCK), dtype)

    gathered, new_outer, new_momentum = pl.pallas_call(
        kernel,
        out_shape=(blocks(NX * NY), blocks(dtype=F32), blocks(dtype=F32)),
        in_specs=[any_space, scalars, scalars, any_space, any_space],
        out_specs=(vector, vector, vector),
        scratch_shapes=[
            blocks(NX * NY),
            blocks(NY, NX),
            blocks(NX),
            blocks(NX),
            blocks(NY),
            blocks(NY),
            blocks(NY),
            blocks(NY),
            blocks(NX),
            blocks(NY),
            blocks(NY),
            blocks(dtype=F32),
            blocks(dtype=F32),
            pltpu.SemaphoreType.DMA((NX * NY + 2,)),
            pltpu.SemaphoreType.DMA((COPIES,)),
            pltpu.SemaphoreType.DMA((COPIES,)),
        ],
        compiler_params=pltpu.CompilerParams(collective_id=0, has_side_effects=True),
        name="outer_step",
    )(deltas, presence, owner_of, outer_params, momentum)
    in_vmem = functools.partial(pltpu.with_memory_space_constraint, memory_space=pltpu.VMEM)
    return pl.pallas_call(
        place_kernel,
        out_shape=(
            jax.ShapeDtypeStruct((rows, width), BF16),
            jax.ShapeDtypeStruct((rows, BLOCK), F32),
            jax.ShapeDtypeStruct((rows, BLOCK), F32),
        ),
        in_specs=[scalars, vector, vector, vector],
        out_specs=(any_space, any_space, any_space),
        scratch_shapes=[pltpu.SemaphoreType.DMA((NX * NY + 2,))],
        name="place_blocks",
    )(owner_of, in_vmem(gathered), in_vmem(new_outer), in_vmem(new_momentum))


def solution(mesh):
    return jax.shard_map(
        shards,
        mesh=mesh,
        in_specs=(P("rep", "shard", None), P(), P(), P("shard", "rep"), P("shard", "rep")),
        out_specs=(P("shard", None), P("shard", "rep"), P("shard", "rep")),
        check_vma=False,
    )
```

```python
import functools

import jax
import jax.numpy as jnp
from jax import lax
from jax.experimental import pallas as pl
from jax.experimental.pallas import tpu as pltpu
from jax.sharding import PartitionSpec as P

PLAN = ('F40', 'F30', 'F50', 'F60', 'F20', 'S00', 'N40', 'N50', 'N30', 'N60', 'N20', 'F41', 'F31', 'F51', 'F61', 'F21', 'S01', 'N41', 'N51', 'N31', 'N61', 'N21', 'T00', 'T40', 'T30', 'T50', 'T20', 'T60', 'T01', 'T41', 'T31', 'T51', 'T21', 'T61', 'M50', 'M30', 'M60', 'M20', 'O00', 'Y40', 'M51', 'M31', 'M61', 'M21', 'Y30', 'Y50', 'Y60', 'Y20', 'O01', 'Y41', 'Y31', 'Y51', 'L00', 'Y61', 'Y21', 'D00', 'D01', 'A60', 'A20', 'G00', 'A50', 'A30', 'A40', 'A61', 'A21', 'G01', 'A51', 'A31', 'A41', 'E00', 'E01')
PARTS = 2
MESH = pl.DeviceIdType.MESH
NX, NY = 4, 8
BLOCK = 128
SLABS = 4
COPIES = 60 * PARTS
UP = (4, 3, 2)
F32, BF16 = jnp.float32, jnp.bfloat16


def kernel(
    deltas, presence, owner_of, outer_in, momentum_in,
    gathered, outer_out, momentum_out,
    delta, buf, side_up, side_down, near_l, near_r, far, mixed, row_out,
    to_y, from_y, outer_v, momentum_v,
    load_sem, send_sems, recv_sems,
):
    me = lax.axis_index("rep")
    x = me // NY
    y = me % NY

    def place(dx, dy):
        return ((x + dx) % NX) * NY + (y + dy) % NY

    right, left = place(1, 0), place(3, 0)
    across, up, down = place(2, 0), place(0, 1), place(0, 7)

    loads = [
        pltpu.make_async_copy(deltas.at[0, :, b * BLOCK : (b + 1) * BLOCK], delta.at[b], load_sem.at[b])
        for b in range(NX * NY)
    ]
    for load in loads:
        load.start()
    load_outer = pltpu.make_async_copy(outer_in, outer_v, load_sem.at[NX * NY])
    load_momentum = pltpu.make_async_copy(momentum_in, momentum_v, load_sem.at[NX * NY + 1])
    load_outer.start()
    load_momentum.start()

    barrier = pltpu.get_barrier_semaphore()
    partners = [right, left, across] + [place(0, dy) for dy in range(1, NY)]
    for partner in partners:
        pl.semaphore_signal(barrier, inc=1, device_id={"rep": partner}, device_id_type=MESH)

    present = presence[me].astype(F32)
    for load in loads:
        load.wait()

    masked = set()
    height = BLOCK // PARTS

    def rows_of(h):
        return pl.ds(h * height, height)

    def term(dy, dx, h):
        rows = rows_of(h)
        if (dy, dx, h) not in masked:
            masked.add((dy, dx, h))
            block = delta[owner_of[place(dx, dy)]][h * height : (h + 1) * height]
            buf[dy, dx, rows] = (block.astype(F32) * present).astype(BF16)
        return buf.at[dy, dx, rows]

    started = []

    def send(src, dst, to):
        k = len(started)
        copy = pltpu.make_async_remote_copy(
            src_ref=src, dst_ref=dst, send_sem=send_sems.at[k], recv_sem=recv_sems.at[k],
            device_id={"rep": to}, device_id_type=MESH,
        )
        copy.start()
        started.append(copy)
        return copy

    def drain():
        for copy in started:
            copy.wait_send()

    c = {}
    count = presence[0]
    for r in range(1, NX * NY):
        count = count + presence[r]

    def wide(ref):
        return ref[...].astype(F32)

    def own_row(dx, h):
        rows = rows_of(h)
        return wide(term(0, dx, h)) + (wide(side_up.at[dx, rows]) + wide(side_down.at[dx, rows]))

    def block_ref(dx, dy, h):
        return gathered.at[place(dx, dy), rows_of(h)]

    def forward(dx, dy, h, to):
        ref = block_ref(dx, dy, h)
        return send(ref, ref, to)

    def spread(dy, h):
        c["right", dy, h] = forward(0, dy, h, right)
        c["left", dy, h] = forward(0, dy, h, left)
        c["across", dy, h] = forward(0, dy, h, across)

    def finish_sum(h):
        rows = rows_of(h)
        total = own_row(0, h)
        for dx in (1, 2, 3):
            c["own", dx, h].wait_recv()
        total = total + (wide(near_l.at[0, rows]) + wide(near_r.at[0, rows]) + wide(far.at[0, rows]))
        for dy in (4, 3, 5, 6, 2):
            c["y", dy, h].wait_recv()
            total = total + wide(from_y.at[dy, rows])
        average = total / count.astype(F32)
        new_momentum = 0.9 * momentum_v[rows] + average
        new_outer = outer_v[rows] - 0.7 * (average + 0.9 * new_momentum)
        gathered[me, rows] = new_outer.astype(BF16)
        for dy in (2, 6, 0, 3, 5, 4, 1, 7):
            if dy:
                c["fan", dy, h] = forward(0, 0, h, place(0, dy))
            else:
                spread(0, h)
        outer_out[rows] = new_outer
        momentum_out[rows] = new_momentum

    def do_step(step, dy, h):
        rows = rows_of(h)
        if step == "F":
            to = across if dy == 4 else right if dy in UP else left
            c["far", dy, h] = send(term(dy, 2, h), far.at[dy, rows], to)
        elif step == "N":
            if dy == 4 or dy not in UP:
                c["l", dy, h] = send(term(dy, 1, h), near_l.at[dy, rows], right)
            if dy in UP:
                c["r", dy, h] = send(term(dy, 3, h), near_r.at[dy, rows], left)
        elif step == "M":
            own_term = wide(term(dy, 1 if dy in UP else 3, h))
            c["far", dy, h].wait_recv()
            mixed[dy, rows] = (wide(far.at[dy, rows]) + own_term).astype(BF16)
            if dy in UP:
                c["l", dy, h] = send(mixed.at[dy, rows], near_l.at[dy, rows], right)
            else:
                c["r", dy, h] = send(mixed.at[dy, rows], near_r.at[dy, rows], left)
        elif step == "S":
            for src, dst, to in ((1, side_up, up), (7, side_down, down)):
                for dx in range(NX):
                    term(src, dx, h)
                c["side", src, h] = send(buf.at[src, :, rows], dst.at[:, rows], to)
        elif step == "O":
            c["side", 1, h].wait_recv()
            c["side", 7, h].wait_recv()
            for dx, dst, to in ((2, far, across), (1, near_l, right), (3, near_r, left)):
                row_out[dx, rows] = own_row(dx, h).astype(BF16)
                c["own", dx, h] = send(row_out.at[dx, rows], dst.at[0, rows], to)
        elif step == "T":
            term(dy, 0, h)
            if dy == 0:
                for dx in range(NX):
                    term(0, dx, h)
            elif dy != 4:
                term(dy, 1 if dy in UP else 3, h)
        elif step == "Y":
            own_term = wide(term(dy, 0, h))
            c["l", dy, h].wait_recv()
            c["r", dy, h].wait_recv()
            x_total = own_term + (wide(near_l.at[dy, rows]) + wide(near_r.at[dy, rows]))
            if dy == 4:
                c["far", dy, h].wait_recv()
                x_total = x_total + wide(far.at[dy, rows])
            to_y[dy, rows] = x_total.astype(BF16)
            c["y", dy, h] = send(to_y.at[dy, rows], from_y.at[dy, rows], place(0, dy))
        elif step == "L":
            load_outer.wait()
            load_momentum.wait()
        elif step == "D":
            finish_sum(h)
        elif step == "A":
            c["fan", NY - dy, h].wait_recv()
            spread(dy, h)
        elif step == "G":
            for name, dx in (("left", 1), ("right", 3), ("across", 2)):
                c[name, 0, h].wait_recv()
                c["side_up", dx, h] = forward(dx, 0, h, up)
                c["side_down", dx, h] = forward(dx, 0, h, down)
        elif step == "E":
            c["fan", 1, h].wait_recv()
            c["fan", 7, h].wait_recv()
            for dy in (6, 2, 5, 3, 4):
                for name in ("right", "left", "across"):
                    c[name, dy, h].wait_recv()
            for dx in (1, 2, 3):
                c["side_up", dx, h].wait_recv()
                c["side_down", dx, h].wait_recv()

    pl.semaphore_wait(barrier, len(partners))
    for token in PLAN:
        do_step(token[0], int(token[1]), int(token[2]))
    drain()
    assert len(started) <= COPIES


def place_kernel(owner_of, gathered, outer_v, momentum_v, weights_out, outer_out, momentum_out, natural, sems):
    copies = [
        pltpu.make_async_copy(outer_v, outer_out, sems.at[SLABS]),
        pltpu.make_async_copy(momentum_v, momentum_out, sems.at[SLABS + 1]),
    ]
    for copy in copies:
        copy.start()
    for slab in range(SLABS):
        rows = pl.ds(slab * (BLOCK // SLABS), BLOCK // SLABS)
        for j in range(NX * NY):
            columns = pl.ds(pl.multiple_of(owner_of[j] * BLOCK, BLOCK), BLOCK)
            natural[rows, columns] = gathered[j, rows]
        copy = pltpu.make_async_copy(natural.at[rows], weights_out.at[rows], sems.at[slab])
        copy.start()
        copies.append(copy)
    for copy in copies:
        copy.wait()


def shards(deltas, presence, owner_of, outer_params, momentum):
    rows, width = deltas.shape[1], deltas.shape[2]
    any_space = pl.BlockSpec(memory_space=pl.ANY)
    scalars = pl.BlockSpec(memory_space=pltpu.SMEM)
    vector = pl.BlockSpec(memory_space=pltpu.VMEM)

    def blocks(*shape, dtype=BF16):
        return pltpu.VMEM((*shape, rows, BLOCK), dtype)

    gathered, new_outer, new_momentum = pl.pallas_call(
        kernel,
        out_shape=(blocks(NX * NY), blocks(dtype=F32), blocks(dtype=F32)),
        in_specs=[any_space, scalars, scalars, any_space, any_space],
        out_specs=(vector, vector, vector),
        scratch_shapes=[
            blocks(NX * NY),
            blocks(NY, NX),
            blocks(NX),
            blocks(NX),
            blocks(NY),
            blocks(NY),
            blocks(NY),
            blocks(NY),
            blocks(NX),
            blocks(NY),
            blocks(NY),
            blocks(dtype=F32),
            blocks(dtype=F32),
            pltpu.SemaphoreType.DMA((NX * NY + 2,)),
            pltpu.SemaphoreType.DMA((COPIES,)),
            pltpu.SemaphoreType.DMA((COPIES,)),
        ],
        compiler_params=pltpu.CompilerParams(collective_id=0, has_side_effects=True),
        name="outer_step",
    )(deltas, presence, owner_of, outer_params, momentum)
    in_vmem = functools.partial(pltpu.with_memory_space_constraint, memory_space=pltpu.VMEM)
    return pl.pallas_call(
        place_kernel,
        out_shape=(
            jax.ShapeDtypeStruct((rows, width), BF16),
            jax.ShapeDtypeStruct((rows, BLOCK), F32),
            jax.ShapeDtypeStruct((rows, BLOCK), F32),
        ),
        in_specs=[scalars, vector, vector, vector],
        out_specs=(any_space, any_space, any_space),
        scratch_shapes=[pltpu.VMEM((rows, width), BF16), pltpu.SemaphoreType.DMA((SLABS + 2,))],
        name="place_blocks",
    )(owner_of, in_vmem(gathered), in_vmem(new_outer), in_vmem(new_momentum))


def solution(mesh):
    return jax.shard_map(
        shards,
        mesh=mesh,
        in_specs=(P("rep", "shard", None), P(), P(), P("shard", "rep"), P("shard", "rep")),
        out_specs=(P("shard", None), P("shard", "rep"), P("shard", "rep")),
        check_vma=False,
    )
```

```python
import functools

import jax
import jax.numpy as jnp
from jax import lax
from jax.experimental import pallas as pl
from jax.experimental.pallas import tpu as pltpu
from jax.sharding import PartitionSpec as P

PLAN = ('F40', 'F30', 'S00', 'F50', 'F60', 'F20', 'N40', 'N50', 'N30', 'N60', 'N20', 'F41', 'F31', 'S01', 'F51', 'F61', 'F21', 'N41', 'N51', 'N31', 'N61', 'N21', 'T00', 'T40', 'T30', 'T50', 'T20', 'T60', 'T01', 'T41', 'T31', 'T51', 'T21', 'T61', 'M50', 'M30', 'M60', 'M20', 'O00', 'H00', 'Y40', 'M51', 'M31', 'M61', 'M21', 'Y30', 'Y50', 'Y60', 'Y20', 'O01', 'Y41', 'Y31', 'Y51', 'L00', 'Y61', 'Y21', 'D00', 'D01', 'A60', 'A20', 'G00', 'A50', 'A30', 'A40', 'A61', 'A21', 'G01', 'A51', 'A31', 'A41', 'E00', 'E01')
PARTS = 2
MESH = pl.DeviceIdType.MESH
NX, NY = 4, 8
BLOCK = 128
SLABS = 4
COPIES = 60 * PARTS
UP = (4, 3, 2)
F32, BF16 = jnp.float32, jnp.bfloat16


def kernel(
    deltas, presence, owner_of, outer_in, momentum_in,
    gathered, outer_out, momentum_out,
    delta, buf, side_up, side_down, near_l, near_r, far, mixed, row_out,
    to_y, from_y, outer_v, momentum_v,
    load_sem, send_sems, recv_sems, ready_sem,
):
    me = lax.axis_index("rep")
    x = me // NY
    y = me % NY

    def place(dx, dy):
        return ((x + dx) % NX) * NY + (y + dy) % NY

    right, left = place(1, 0), place(3, 0)
    across, up, down = place(2, 0), place(0, 1), place(0, 7)

    loads = [
        pltpu.make_async_copy(deltas.at[0, :, b * BLOCK : (b + 1) * BLOCK], delta.at[b], load_sem.at[b])
        for b in range(NX * NY)
    ]
    for load in loads:
        load.start()
    load_outer = pltpu.make_async_copy(outer_in, outer_v, load_sem.at[NX * NY])
    load_momentum = pltpu.make_async_copy(momentum_in, momentum_v, load_sem.at[NX * NY + 1])
    load_outer.start()
    load_momentum.start()

    barrier = pltpu.get_barrier_semaphore()
    near = (1, 2, 6, 7)
    partners = [right, left, across] + [place(0, dy) for dy in near]
    for partner in partners:
        pl.semaphore_signal(barrier, inc=1, device_id={"rep": partner}, device_id_type=MESH)

    present = presence[me].astype(F32)
    for load in loads:
        load.wait()

    masked = set()
    height = BLOCK // PARTS

    def rows_of(h):
        return pl.ds(h * height, height)

    def term(dy, dx, h):
        rows = rows_of(h)
        if (dy, dx, h) not in masked:
            masked.add((dy, dx, h))
            block = delta[owner_of[place(dx, dy)]][h * height : (h + 1) * height]
            buf[dy, dx, rows] = (block.astype(F32) * present).astype(BF16)
        return buf.at[dy, dx, rows]

    started = []

    def send(src, dst, to):
        k = len(started)
        copy = pltpu.make_async_remote_copy(
            src_ref=src, dst_ref=dst, send_sem=send_sems.at[k], recv_sem=recv_sems.at[k],
            device_id={"rep": to}, device_id_type=MESH,
        )
        copy.start()
        started.append(copy)
        return copy

    def drain():
        for copy in started:
            copy.wait_send()

    c = {}
    count = presence[0]
    for r in range(1, NX * NY):
        count = count + presence[r]

    def wide(ref):
        return ref[...].astype(F32)

    def own_row(dx, h):
        rows = rows_of(h)
        return wide(term(0, dx, h)) + (wide(side_up.at[dx, rows]) + wide(side_down.at[dx, rows]))

    def block_ref(dx, dy, h):
        return gathered.at[place(dx, dy), rows_of(h)]

    def forward(dx, dy, h, to):
        ref = block_ref(dx, dy, h)
        return send(ref, ref, to)

    def spread(dy, h):
        c["right", dy, h] = forward(0, dy, h, right)
        c["left", dy, h] = forward(0, dy, h, left)
        c["across", dy, h] = forward(0, dy, h, across)

    def finish_sum(h):
        rows = rows_of(h)
        total = own_row(0, h)
        for dx in (1, 2, 3):
            c["own", dx, h].wait_recv()
        total = total + (wide(near_l.at[0, rows]) + wide(near_r.at[0, rows]) + wide(far.at[0, rows]))
        for dy in (4, 3, 5, 6, 2):
            c["y", dy, h].wait_recv()
            total = total + wide(from_y.at[dy, rows])
        average = total / count.astype(F32)
        new_momentum = 0.9 * momentum_v[rows] + average
        new_outer = outer_v[rows] - 0.7 * (average + 0.9 * new_momentum)
        gathered[me, rows] = new_outer.astype(BF16)
        for dy in (2, 6, 0, 3, 5, 4, 1, 7):
            if dy:
                c["fan", dy, h] = forward(0, 0, h, place(0, dy))
            else:
                spread(0, h)
        outer_out[rows] = new_outer
        momentum_out[rows] = new_momentum

    def do_step(step, dy, h):
        rows = rows_of(h)
        if step == "F":
            to = across if dy == 4 else right if dy in UP else left
            c["far", dy, h] = send(term(dy, 2, h), far.at[dy, rows], to)
        elif step == "N":
            if dy == 4 or dy not in UP:
                c["l", dy, h] = send(term(dy, 1, h), near_l.at[dy, rows], right)
            if dy in UP:
                c["r", dy, h] = send(term(dy, 3, h), near_r.at[dy, rows], left)
        elif step == "M":
            own_term = wide(term(dy, 1 if dy in UP else 3, h))
            c["far", dy, h].wait_recv()
            mixed[dy, rows] = (wide(far.at[dy, rows]) + own_term).astype(BF16)
            if dy in UP:
                c["l", dy, h] = send(mixed.at[dy, rows], near_l.at[dy, rows], right)
            else:
                c["r", dy, h] = send(mixed.at[dy, rows], near_r.at[dy, rows], left)
        elif step == "S":
            for src, dst, to in ((1, side_up, up), (7, side_down, down)):
                for dx in range(NX):
                    term(src, dx, h)
                c["side", src, h] = send(buf.at[src, :, rows], dst.at[:, rows], to)
        elif step == "O":
            c["side", 1, h].wait_recv()
            c["side", 7, h].wait_recv()
            for dx, dst, to in ((2, far, across), (1, near_l, right), (3, near_r, left)):
                row_out[dx, rows] = own_row(dx, h).astype(BF16)
                c["own", dx, h] = send(row_out.at[dx, rows], dst.at[0, rows], to)
        elif step == "T":
            term(dy, 0, h)
            if dy == 0:
                for dx in range(NX):
                    term(0, dx, h)
            elif dy != 4:
                term(dy, 1 if dy in UP else 3, h)
        elif step == "Y":
            own_term = wide(term(dy, 0, h))
            c["l", dy, h].wait_recv()
            c["r", dy, h].wait_recv()
            x_total = own_term + (wide(near_l.at[dy, rows]) + wide(near_r.at[dy, rows]))
            if dy == 4:
                c["far", dy, h].wait_recv()
                x_total = x_total + wide(far.at[dy, rows])
            to_y[dy, rows] = x_total.astype(BF16)
            c["y", dy, h] = send(to_y.at[dy, rows], from_y.at[dy, rows], place(0, dy))
        elif step == "H":
            pl.semaphore_wait(ready_sem, 2)
        elif step == "L":
            load_outer.wait()
            load_momentum.wait()
        elif step == "D":
            finish_sum(h)
        elif step == "A":
            c["fan", NY - dy, h].wait_recv()
            spread(dy, h)
        elif step == "G":
            for name, dx in (("left", 1), ("right", 3), ("across", 2)):
                c[name, 0, h].wait_recv()
                c["side_up", dx, h] = forward(dx, 0, h, up)
                c["side_down", dx, h] = forward(dx, 0, h, down)
        elif step == "E":
            c["fan", 1, h].wait_recv()
            c["fan", 7, h].wait_recv()
            for dy in (6, 2, 5, 3, 4):
                for name in ("right", "left", "across"):
                    c[name, dy, h].wait_recv()
            for dx in (1, 2, 3):
                c["side_up", dx, h].wait_recv()
                c["side_down", dx, h].wait_recv()

    pl.semaphore_wait(barrier, len(partners))
    for dy in (2, 6):
        pl.semaphore_signal(ready_sem, inc=1, device_id={"rep": place(0, dy)}, device_id_type=MESH)
    for token in PLAN:
        do_step(token[0], int(token[1]), int(token[2]))
    drain()
    assert len(started) <= COPIES


def place_kernel(owner_of, gathered, outer_v, momentum_v, weights_out, outer_out, momentum_out, natural, sems):
    copies = [
        pltpu.make_async_copy(outer_v, outer_out, sems.at[SLABS]),
        pltpu.make_async_copy(momentum_v, momentum_out, sems.at[SLABS + 1]),
    ]
    for copy in copies:
        copy.start()
    for slab in range(SLABS):
        rows = pl.ds(slab * (BLOCK // SLABS), BLOCK // SLABS)
        for j in range(NX * NY):
            columns = pl.ds(pl.multiple_of(owner_of[j] * BLOCK, BLOCK), BLOCK)
            natural[rows, columns] = gathered[j, rows]
        copy = pltpu.make_async_copy(natural.at[rows], weights_out.at[rows], sems.at[slab])
        copy.start()
        copies.append(copy)
    for copy in copies:
        copy.wait()


def shards(deltas, presence, owner_of, outer_params, momentum):
    rows, width = deltas.shape[1], deltas.shape[2]
    any_space = pl.BlockSpec(memory_space=pl.ANY)
    scalars = pl.BlockSpec(memory_space=pltpu.SMEM)
    vector = pl.BlockSpec(memory_space=pltpu.VMEM)

    def blocks(*shape, dtype=BF16):
        return pltpu.VMEM((*shape, rows, BLOCK), dtype)

    gathered, new_outer, new_momentum = pl.pallas_call(
        kernel,
        out_shape=(blocks(NX * NY), blocks(dtype=F32), blocks(dtype=F32)),
        in_specs=[any_space, scalars, scalars, any_space, any_space],
        out_specs=(vector, vector, vector),
        scratch_shapes=[
            blocks(NX * NY),
            blocks(NY, NX),
            blocks(NX),
            blocks(NX),
            blocks(NY),
            blocks(NY),
            blocks(NY),
            blocks(NY),
            blocks(NX),
            blocks(NY),
            blocks(NY),
            blocks(dtype=F32),
            blocks(dtype=F32),
            pltpu.SemaphoreType.DMA((NX * NY + 2,)),
            pltpu.SemaphoreType.DMA((COPIES,)),
            pltpu.SemaphoreType.DMA((COPIES,)),
            pltpu.SemaphoreType.REGULAR,
        ],
        compiler_params=pltpu.CompilerParams(collective_id=0, has_side_effects=True),
        name="outer_step",
    )(deltas, presence, owner_of, outer_params, momentum)
    in_vmem = functools.partial(pltpu.with_memory_space_constraint, memory_space=pltpu.VMEM)
    return pl.pallas_call(
        place_kernel,
        out_shape=(
            jax.ShapeDtypeStruct((rows, width), BF16),
            jax.ShapeDtypeStruct((rows, BLOCK), F32),
            jax.ShapeDtypeStruct((rows, BLOCK), F32),
        ),
        in_specs=[scalars, vector, vector, vector],
        out_specs=(any_space, any_space, any_space),
        scratch_shapes=[pltpu.VMEM((rows, width), BF16), pltpu.SemaphoreType.DMA((SLABS + 2,))],
        name="place_blocks",
    )(owner_of, in_vmem(gathered), in_vmem(new_outer), in_vmem(new_momentum))


def solution(mesh):
    return jax.shard_map(
        shards,
        mesh=mesh,
        in_specs=(P("rep", "shard", None), P(), P(), P("shard", "rep"), P("shard", "rep")),
        out_specs=(P("shard", None), P("shard", "rep"), P("shard", "rep")),
        check_vma=False,
    )
```

```python
import functools

import jax
import jax.numpy as jnp
from jax import lax
from jax.experimental import pallas as pl
from jax.experimental.pallas import tpu as pltpu
from jax.sharding import PartitionSpec as P

PLAN = ('F30', 'S00', 'F50', 'F60', 'F20', 'N40', 'N50', 'N30', 'N60', 'N20', 'I00', 'F40', 'F31', 'S01', 'F51', 'F61', 'F21', 'N41', 'N51', 'N31', 'N61', 'N21', 'F41', 'T00', 'T40', 'T30', 'T50', 'T20', 'T60', 'T01', 'T41', 'T31', 'T51', 'T21', 'T61', 'M50', 'M30', 'M60', 'M20', 'O00', 'H00', 'Y40', 'M51', 'M31', 'M61', 'M21', 'Y30', 'Y50', 'Y60', 'Y20', 'O01', 'Y41', 'Y31', 'Y51', 'L00', 'Y61', 'Y21', 'D00', 'D01', 'A60', 'A20', 'G00', 'A50', 'A30', 'A40', 'A61', 'A21', 'G01', 'A51', 'A31', 'A41', 'E00', 'E01')
PARTS = 2
MESH = pl.DeviceIdType.MESH
NX, NY = 4, 8
BLOCK = 128
SLABS = 4
COPIES = 60 * PARTS
UP = (4, 3, 2)
F32, BF16 = jnp.float32, jnp.bfloat16


def kernel(
    deltas, presence, owner_of, outer_in, momentum_in,
    gathered, outer_out, momentum_out,
    delta, buf, side_up, side_down, near_l, near_r, far, mixed, row_out,
    to_y, from_y, outer_v, momentum_v,
    load_sem, send_sems, recv_sems, ready_sem, far_sem,
):
    me = lax.axis_index("rep")
    x = me // NY
    y = me % NY

    def place(dx, dy):
        return ((x + dx) % NX) * NY + (y + dy) % NY

    right, left = place(1, 0), place(3, 0)
    across, up, down = place(2, 0), place(0, 1), place(0, 7)

    loads = [
        pltpu.make_async_copy(deltas.at[0, :, b * BLOCK : (b + 1) * BLOCK], delta.at[b], load_sem.at[b])
        for b in range(NX * NY)
    ]
    for load in loads:
        load.start()
    load_outer = pltpu.make_async_copy(outer_in, outer_v, load_sem.at[NX * NY])
    load_momentum = pltpu.make_async_copy(momentum_in, momentum_v, load_sem.at[NX * NY + 1])
    load_outer.start()
    load_momentum.start()

    barrier = pltpu.get_barrier_semaphore()
    partners = [right, left, up, down]
    for partner in partners:
        pl.semaphore_signal(barrier, inc=1, device_id={"rep": partner}, device_id_type=MESH)

    present = presence[me].astype(F32)
    for load in loads:
        load.wait()

    masked = set()
    height = BLOCK // PARTS

    def rows_of(h):
        return pl.ds(h * height, height)

    def term(dy, dx, h):
        rows = rows_of(h)
        if (dy, dx, h) not in masked:
            masked.add((dy, dx, h))
            block = delta[owner_of[place(dx, dy)]][h * height : (h + 1) * height]
            buf[dy, dx, rows] = (block.astype(F32) * present).astype(BF16)
        return buf.at[dy, dx, rows]

    started = []

    def send(src, dst, to):
        k = len(started)
        copy = pltpu.make_async_remote_copy(
            src_ref=src, dst_ref=dst, send_sem=send_sems.at[k], recv_sem=recv_sems.at[k],
            device_id={"rep": to}, device_id_type=MESH,
        )
        copy.start()
        started.append(copy)
        return copy

    def drain():
        for copy in started:
            copy.wait_send()

    c = {}
    count = presence[0]
    for r in range(1, NX * NY):
        count = count + presence[r]

    def wide(ref):
        return ref[...].astype(F32)

    def own_row(dx, h):
        rows = rows_of(h)
        return wide(term(0, dx, h)) + (wide(side_up.at[dx, rows]) + wide(side_down.at[dx, rows]))

    def block_ref(dx, dy, h):
        return gathered.at[place(dx, dy), rows_of(h)]

    def forward(dx, dy, h, to):
        ref = block_ref(dx, dy, h)
        return send(ref, ref, to)

    def spread(dy, h):
        c["right", dy, h] = forward(0, dy, h, right)
        c["left", dy, h] = forward(0, dy, h, left)
        c["across", dy, h] = forward(0, dy, h, across)

    def finish_sum(h):
        rows = rows_of(h)
        total = own_row(0, h)
        for dx in (1, 2, 3):
            c["own", dx, h].wait_recv()
        total = total + (wide(near_l.at[0, rows]) + wide(near_r.at[0, rows]) + wide(far.at[0, rows]))
        for dy in (4, 3, 5, 6, 2):
            c["y", dy, h].wait_recv()
            total = total + wide(from_y.at[dy, rows])
        average = total / count.astype(F32)
        new_momentum = 0.9 * momentum_v[rows] + average
        new_outer = outer_v[rows] - 0.7 * (average + 0.9 * new_momentum)
        gathered[me, rows] = new_outer.astype(BF16)
        for dy in (2, 6, 0, 3, 5, 4, 1, 7):
            if dy:
                c["fan", dy, h] = forward(0, 0, h, place(0, dy))
            else:
                spread(0, h)
        outer_out[rows] = new_outer
        momentum_out[rows] = new_momentum

    def do_step(step, dy, h):
        rows = rows_of(h)
        if step == "F":
            to = across if dy == 4 else right if dy in UP else left
            c["far", dy, h] = send(term(dy, 2, h), far.at[dy, rows], to)
        elif step == "N":
            if dy == 4 or dy not in UP:
                c["l", dy, h] = send(term(dy, 1, h), near_l.at[dy, rows], right)
            if dy in UP:
                c["r", dy, h] = send(term(dy, 3, h), near_r.at[dy, rows], left)
        elif step == "M":
            own_term = wide(term(dy, 1 if dy in UP else 3, h))
            c["far", dy, h].wait_recv()
            mixed[dy, rows] = (wide(far.at[dy, rows]) + own_term).astype(BF16)
            if dy in UP:
                c["l", dy, h] = send(mixed.at[dy, rows], near_l.at[dy, rows], right)
            else:
                c["r", dy, h] = send(mixed.at[dy, rows], near_r.at[dy, rows], left)
        elif step == "S":
            for src, dst, to in ((1, side_up, up), (7, side_down, down)):
                for dx in range(NX):
                    term(src, dx, h)
                c["side", src, h] = send(buf.at[src, :, rows], dst.at[:, rows], to)
        elif step == "O":
            c["side", 1, h].wait_recv()
            c["side", 7, h].wait_recv()
            for dx, dst, to in ((2, far, across), (1, near_l, right), (3, near_r, left)):
                row_out[dx, rows] = own_row(dx, h).astype(BF16)
                c["own", dx, h] = send(row_out.at[dx, rows], dst.at[0, rows], to)
        elif step == "T":
            term(dy, 0, h)
            if dy == 0:
                for dx in range(NX):
                    term(0, dx, h)
            elif dy != 4:
                term(dy, 1 if dy in UP else 3, h)
        elif step == "Y":
            own_term = wide(term(dy, 0, h))
            c["l", dy, h].wait_recv()
            c["r", dy, h].wait_recv()
            x_total = own_term + (wide(near_l.at[dy, rows]) + wide(near_r.at[dy, rows]))
            if dy == 4:
                c["far", dy, h].wait_recv()
                x_total = x_total + wide(far.at[dy, rows])
            to_y[dy, rows] = x_total.astype(BF16)
            c["y", dy, h] = send(to_y.at[dy, rows], from_y.at[dy, rows], place(0, dy))
        elif step == "I":
            pl.semaphore_wait(ready_sem, len(partners))
            for near in (2, 6):
                pl.semaphore_signal(far_sem, inc=1, device_id={"rep": place(0, near)}, device_id_type=MESH)
        elif step == "H":
            pl.semaphore_wait(far_sem, 2)
        elif step == "L":
            load_outer.wait()
            load_momentum.wait()
        elif step == "D":
            finish_sum(h)
        elif step == "A":
            c["fan", NY - dy, h].wait_recv()
            spread(dy, h)
        elif step == "G":
            for name, dx in (("left", 1), ("right", 3), ("across", 2)):
                c[name, 0, h].wait_recv()
                c["side_up", dx, h] = forward(dx, 0, h, up)
                c["side_down", dx, h] = forward(dx, 0, h, down)
        elif step == "E":
            c["fan", 1, h].wait_recv()
            c["fan", 7, h].wait_recv()
            for dy in (6, 2, 5, 3, 4):
                for name in ("right", "left", "across"):
                    c[name, dy, h].wait_recv()
            for dx in (1, 2, 3):
                c["side_up", dx, h].wait_recv()
                c["side_down", dx, h].wait_recv()

    pl.semaphore_wait(barrier, len(partners))
    for partner in partners:
        pl.semaphore_signal(ready_sem, inc=1, device_id={"rep": partner}, device_id_type=MESH)
    for token in PLAN:
        do_step(token[0], int(token[1]), int(token[2]))
    drain()
    assert len(started) <= COPIES


def place_kernel(owner_of, gathered, outer_v, momentum_v, weights_out, outer_out, momentum_out, natural, sems):
    copies = [
        pltpu.make_async_copy(outer_v, outer_out, sems.at[SLABS]),
        pltpu.make_async_copy(momentum_v, momentum_out, sems.at[SLABS + 1]),
    ]
    for copy in copies:
        copy.start()
    for slab in range(SLABS):
        rows = pl.ds(slab * (BLOCK // SLABS), BLOCK // SLABS)
        for j in range(NX * NY):
            columns = pl.ds(pl.multiple_of(owner_of[j] * BLOCK, BLOCK), BLOCK)
            natural[rows, columns] = gathered[j, rows]
        copy = pltpu.make_async_copy(natural.at[rows], weights_out.at[rows], sems.at[slab])
        copy.start()
        copies.append(copy)
    for copy in copies:
        copy.wait()


def shards(deltas, presence, owner_of, outer_params, momentum):
    rows, width = deltas.shape[1], deltas.shape[2]
    any_space = pl.BlockSpec(memory_space=pl.ANY)
    scalars = pl.BlockSpec(memory_space=pltpu.SMEM)
    vector = pl.BlockSpec(memory_space=pltpu.VMEM)

    def blocks(*shape, dtype=BF16):
        return pltpu.VMEM((*shape, rows, BLOCK), dtype)

    gathered, new_outer, new_momentum = pl.pallas_call(
        kernel,
        out_shape=(blocks(NX * NY), blocks(dtype=F32), blocks(dtype=F32)),
        in_specs=[any_space, scalars, scalars, any_space, any_space],
        out_specs=(vector, vector, vector),
        scratch_shapes=[
            blocks(NX * NY),
            blocks(NY, NX),
            blocks(NX),
            blocks(NX),
            blocks(NY),
            blocks(NY),
            blocks(NY),
            blocks(NY),
            blocks(NX),
            blocks(NY),
            blocks(NY),
            blocks(dtype=F32),
            blocks(dtype=F32),
            pltpu.SemaphoreType.DMA((NX * NY + 2,)),
            pltpu.SemaphoreType.DMA((COPIES,)),
            pltpu.SemaphoreType.DMA((COPIES,)),
            pltpu.SemaphoreType.REGULAR,
            pltpu.SemaphoreType.REGULAR,
        ],
        compiler_params=pltpu.CompilerParams(collective_id=0, has_side_effects=True),
        name="outer_step",
    )(deltas, presence, owner_of, outer_params, momentum)
    in_vmem = functools.partial(pltpu.with_memory_space_constraint, memory_space=pltpu.VMEM)
    return pl.pallas_call(
        place_kernel,
        out_shape=(
            jax.ShapeDtypeStruct((rows, width), BF16),
            jax.ShapeDtypeStruct((rows, BLOCK), F32),
            jax.ShapeDtypeStruct((rows, BLOCK), F32),
        ),
        in_specs=[scalars, vector, vector, vector],
        out_specs=(any_space, any_space, any_space),
        scratch_shapes=[pltpu.VMEM((rows, width), BF16), pltpu.SemaphoreType.DMA((SLABS + 2,))],
        name="place_blocks",
    )(owner_of, in_vmem(gathered), in_vmem(new_outer), in_vmem(new_momentum))


def solution(mesh):
    return jax.shard_map(
        shards,
        mesh=mesh,
        in_specs=(P("rep", "shard", None), P(), P(), P("shard", "rep"), P("shard", "rep")),
        out_specs=(P("shard", None), P("shard", "rep"), P("shard", "rep")),
        check_vma=False,
    )
```

```python
import functools

import jax
import jax.numpy as jnp
from jax import lax
from jax.experimental import pallas as pl
from jax.experimental.pallas import tpu as pltpu
from jax.sharding import PartitionSpec as P

PLAN = ('F40', 'F30', 'S00', 'F50', 'F60', 'F20', 'N40', 'N50', 'N30', 'N60', 'N20', 'F41', 'F31', 'S01', 'F51', 'F61', 'F21', 'N41', 'N51', 'N31', 'N61', 'N21', 'T00', 'T40', 'T30', 'T50', 'T20', 'T60', 'T01', 'T41', 'T31', 'T51', 'T21', 'T61', 'M50', 'M30', 'M60', 'M20', 'O00', 'H00', 'Y40', 'M51', 'M31', 'M61', 'M21', 'Y30', 'Y50', 'Y60', 'Y20', 'O01', 'Y41', 'Y31', 'Y51', 'L00', 'Y61', 'Y21', 'D00', 'D01', 'A60', 'A20', 'G00', 'A50', 'A30', 'A40', 'A61', 'A21', 'G01', 'A51', 'A31', 'A41', 'E00', 'E01')
PARTS = 2
MESH = pl.DeviceIdType.MESH
NX, NY = 4, 8
BLOCK = 128
SLABS = 4
COPIES = 60 * PARTS
UP = (4, 3, 2)
F32, BF16 = jnp.float32, jnp.bfloat16


def kernel(
    deltas, presence, owner_of, outer_in, momentum_in,
    gathered, outer_out, momentum_out,
    delta, buf, side_up, side_down, near_l, near_r, far, mixed, row_out,
    to_y, from_y, outer_v, momentum_v,
    load_sem, send_sems, recv_sems, ready_sem,
):
    me = lax.axis_index("rep")
    x = me // NY
    y = me % NY

    def place(dx, dy):
        return ((x + dx) % NX) * NY + (y + dy) % NY

    right, left = place(1, 0), place(3, 0)
    across, up, down = place(2, 0), place(0, 1), place(0, 7)

    barrier = pltpu.get_barrier_semaphore()
    near = (1, 2, 6, 7)
    partners = [right, left, across] + [place(0, dy) for dy in near]
    for partner in partners:
        pl.semaphore_signal(barrier, inc=1, device_id={"rep": partner}, device_id_type=MESH)

    loads = [
        pltpu.make_async_copy(deltas.at[0, :, b * BLOCK : (b + 1) * BLOCK], delta.at[b], load_sem.at[b])
        for b in range(NX * NY)
    ]
    for load in loads:
        load.start()
    load_outer = pltpu.make_async_copy(outer_in, outer_v, load_sem.at[NX * NY])
    load_momentum = pltpu.make_async_copy(momentum_in, momentum_v, load_sem.at[NX * NY + 1])
    load_outer.start()
    load_momentum.start()

    present = presence[me].astype(F32)
    for load in loads:
        load.wait()

    masked = set()
    height = BLOCK // PARTS

    def rows_of(h):
        return pl.ds(h * height, height)

    def term(dy, dx, h):
        rows = rows_of(h)
        if (dy, dx, h) not in masked:
            masked.add((dy, dx, h))
            block = delta[owner_of[place(dx, dy)]][h * height : (h + 1) * height]
            buf[dy, dx, rows] = (block.astype(F32) * present).astype(BF16)
        return buf.at[dy, dx, rows]

    started = []

    def send(src, dst, to):
        k = len(started)
        copy = pltpu.make_async_remote_copy(
            src_ref=src, dst_ref=dst, send_sem=send_sems.at[k], recv_sem=recv_sems.at[k],
            device_id={"rep": to}, device_id_type=MESH,
        )
        copy.start()
        started.append(copy)
        return copy

    def drain():
        for copy in started:
            copy.wait_send()

    c = {}
    count = presence[0]
    for r in range(1, NX * NY):
        count = count + presence[r]

    def wide(ref):
        return ref[...].astype(F32)

    def own_row(dx, h):
        rows = rows_of(h)
        return wide(term(0, dx, h)) + (wide(side_up.at[dx, rows]) + wide(side_down.at[dx, rows]))

    def block_ref(dx, dy, h):
        return gathered.at[place(dx, dy), rows_of(h)]

    def forward(dx, dy, h, to):
        ref = block_ref(dx, dy, h)
        return send(ref, ref, to)

    def spread(dy, h):
        c["right", dy, h] = forward(0, dy, h, right)
        c["left", dy, h] = forward(0, dy, h, left)
        c["across", dy, h] = forward(0, dy, h, across)

    def finish_sum(h):
        rows = rows_of(h)
        total = own_row(0, h)
        for dx in (1, 2, 3):
            c["own", dx, h].wait_recv()
        total = total + (wide(near_l.at[0, rows]) + wide(near_r.at[0, rows]) + wide(far.at[0, rows]))
        for dy in (4, 3, 5, 6, 2):
            c["y", dy, h].wait_recv()
            total = total + wide(from_y.at[dy, rows])
        average = total / count.astype(F32)
        new_momentum = 0.9 * momentum_v[rows] + average
        new_outer = outer_v[rows] - 0.7 * (average + 0.9 * new_momentum)
        gathered[me, rows] = new_outer.astype(BF16)
        for dy in (2, 6, 0, 3, 5, 4, 1, 7):
            if dy:
                c["fan", dy, h] = forward(0, 0, h, place(0, dy))
            else:
                spread(0, h)
        outer_out[rows] = new_outer
        momentum_out[rows] = new_momentum

    def do_step(step, dy, h):
        rows = rows_of(h)
        if step == "F":
            to = across if dy == 4 else right if dy in UP else left
            c["far", dy, h] = send(term(dy, 2, h), far.at[dy, rows], to)
        elif step == "N":
            if dy == 4 or dy not in UP:
                c["l", dy, h] = send(term(dy, 1, h), near_l.at[dy, rows], right)
            if dy in UP:
                c["r", dy, h] = send(term(dy, 3, h), near_r.at[dy, rows], left)
        elif step == "M":
            own_term = wide(term(dy, 1 if dy in UP else 3, h))
            c["far", dy, h].wait_recv()
            mixed[dy, rows] = (wide(far.at[dy, rows]) + own_term).astype(BF16)
            if dy in UP:
                c["l", dy, h] = send(mixed.at[dy, rows], near_l.at[dy, rows], right)
            else:
                c["r", dy, h] = send(mixed.at[dy, rows], near_r.at[dy, rows], left)
        elif step == "S":
            for src, dst, to in ((1, side_up, up), (7, side_down, down)):
                for dx in range(NX):
                    term(src, dx, h)
                c["side", src, h] = send(buf.at[src, :, rows], dst.at[:, rows], to)
        elif step == "O":
            c["side", 1, h].wait_recv()
            c["side", 7, h].wait_recv()
            for dx, dst, to in ((2, far, across), (1, near_l, right), (3, near_r, left)):
                row_out[dx, rows] = own_row(dx, h).astype(BF16)
                c["own", dx, h] = send(row_out.at[dx, rows], dst.at[0, rows], to)
        elif step == "T":
            term(dy, 0, h)
            if dy == 0:
                for dx in range(NX):
                    term(0, dx, h)
            elif dy != 4:
                term(dy, 1 if dy in UP else 3, h)
        elif step == "Y":
            own_term = wide(term(dy, 0, h))
            c["l", dy, h].wait_recv()
            c["r", dy, h].wait_recv()
            x_total = own_term + (wide(near_l.at[dy, rows]) + wide(near_r.at[dy, rows]))
            if dy == 4:
                c["far", dy, h].wait_recv()
                x_total = x_total + wide(far.at[dy, rows])
            to_y[dy, rows] = x_total.astype(BF16)
            c["y", dy, h] = send(to_y.at[dy, rows], from_y.at[dy, rows], place(0, dy))
        elif step == "H":
            pl.semaphore_wait(ready_sem, 2)
        elif step == "L":
            load_outer.wait()
            load_momentum.wait()
        elif step == "D":
            finish_sum(h)
        elif step == "A":
            c["fan", NY - dy, h].wait_recv()
            spread(dy, h)
        elif step == "G":
            for name, dx in (("left", 1), ("right", 3), ("across", 2)):
                c[name, 0, h].wait_recv()
                c["side_up", dx, h] = forward(dx, 0, h, up)
                c["side_down", dx, h] = forward(dx, 0, h, down)
        elif step == "E":
            c["fan", 1, h].wait_recv()
            c["fan", 7, h].wait_recv()
            for dy in (6, 2, 5, 3, 4):
                for name in ("right", "left", "across"):
                    c[name, dy, h].wait_recv()
            for dx in (1, 2, 3):
                c["side_up", dx, h].wait_recv()
                c["side_down", dx, h].wait_recv()

    pl.semaphore_wait(barrier, len(partners))
    for dy in (2, 6):
        pl.semaphore_signal(ready_sem, inc=1, device_id={"rep": place(0, dy)}, device_id_type=MESH)
    for token in PLAN:
        do_step(token[0], int(token[1]), int(token[2]))
    drain()
    assert len(started) <= COPIES


def place_kernel(owner_of, gathered, outer_v, momentum_v, weights_out, outer_out, momentum_out, natural, sems):
    copies = [
        pltpu.make_async_copy(outer_v, outer_out, sems.at[SLABS]),
        pltpu.make_async_copy(momentum_v, momentum_out, sems.at[SLABS + 1]),
    ]
    for copy in copies:
        copy.start()
    for slab in range(SLABS):
        rows = pl.ds(slab * (BLOCK // SLABS), BLOCK // SLABS)
        for j in range(NX * NY):
            columns = pl.ds(pl.multiple_of(owner_of[j] * BLOCK, BLOCK), BLOCK)
            natural[rows, columns] = gathered[j, rows]
        copy = pltpu.make_async_copy(natural.at[rows], weights_out.at[rows], sems.at[slab])
        copy.start()
        copies.append(copy)
    for copy in copies:
        copy.wait()


def shards(deltas, presence, owner_of, outer_params, momentum):
    rows, width = deltas.shape[1], deltas.shape[2]
    any_space = pl.BlockSpec(memory_space=pl.ANY)
    scalars = pl.BlockSpec(memory_space=pltpu.SMEM)
    vector = pl.BlockSpec(memory_space=pltpu.VMEM)

    def blocks(*shape, dtype=BF16):
        return pltpu.VMEM((*shape, rows, BLOCK), dtype)

    gathered, new_outer, new_momentum = pl.pallas_call(
        kernel,
        out_shape=(blocks(NX * NY), blocks(dtype=F32), blocks(dtype=F32)),
        in_specs=[any_space, scalars, scalars, any_space, any_space],
        out_specs=(vector, vector, vector),
        scratch_shapes=[
            blocks(NX * NY),
            blocks(NY, NX),
            blocks(NX),
            blocks(NX),
            blocks(NY),
            blocks(NY),
            blocks(NY),
            blocks(NY),
            blocks(NX),
            blocks(NY),
            blocks(NY),
            blocks(dtype=F32),
            blocks(dtype=F32),
            pltpu.SemaphoreType.DMA((NX * NY + 2,)),
            pltpu.SemaphoreType.DMA((COPIES,)),
            pltpu.SemaphoreType.DMA((COPIES,)),
            pltpu.SemaphoreType.REGULAR,
        ],
        compiler_params=pltpu.CompilerParams(collective_id=0, has_side_effects=True),
        name="outer_step",
    )(deltas, presence, owner_of, outer_params, momentum)
    in_vmem = functools.partial(pltpu.with_memory_space_constraint, memory_space=pltpu.VMEM)
    return pl.pallas_call(
        place_kernel,
        out_shape=(
            jax.ShapeDtypeStruct((rows, width), BF16),
            jax.ShapeDtypeStruct((rows, BLOCK), F32),
            jax.ShapeDtypeStruct((rows, BLOCK), F32),
        ),
        in_specs=[scalars, vector, vector, vector],
        out_specs=(any_space, any_space, any_space),
        scratch_shapes=[pltpu.VMEM((rows, width), BF16), pltpu.SemaphoreType.DMA((SLABS + 2,))],
        name="place_blocks",
    )(owner_of, in_vmem(gathered), in_vmem(new_outer), in_vmem(new_momentum))


def solution(mesh):
    return jax.shard_map(
        shards,
        mesh=mesh,
        in_specs=(P("rep", "shard", None), P(), P(), P("shard", "rep"), P("shard", "rep")),
        out_specs=(P("shard", None), P("shard", "rep"), P("shard", "rep")),
        check_vma=False,
    )
```
